512 devices in a mesh: dp: 64 (over z_lo, x, core), ens: 8 (over y, z_hi).
Axes of the slice: x: 4, y: 4, z: 16 (z_hi: 2, z_lo: 8; z = z_hi * 8 + z_lo), core: 2. Of those that a mesh axis runs over, the one named last changes fastest.
Arguments:
- embeddings: bfloat16 [49152, 1024], P('dp'), may hold values from -6 to 6
- valid_mask: int32 [49152], P('dp'), may hold values 0 or 1
- first_weight: bfloat16 [8, 1024, 4096], P(None, 'dp', 'ens'), may hold values from -0.1875 to 0.1875
- second_weight: bfloat16 [8, 4096, 128], P(None, 'ens'), may hold values from -0.09375 to 0.09375
- thresholds: int32 [8], replicated, may hold values from -256 to 256
Outputs:
- mean_logits: float32 [49152, 128], P('dp')
- kept_share: float32 [8], P('ens')
- agree_share: float32 [8], P('ens')
The draws below stay inside these ranges and needn't reach their ends.
All inputs are finite; a program needn't handle non-finite values. No bound on the sum of `valid_mask` on one device may be relied on, other than what follows from the above.
Results may differ from the reference program's by a relative error of at most 0.0044.
Values may be sent and summed in bfloat16 or wider, within the bound.
A program may use at most 64 MiB of HBM per device.

```python
import jax
import jax.numpy as jnp
from jax import lax

D = 1024
H = 4096
C = 128
DOC_DEV = 768
MEMBERS = 8
DOCS = 49152
N_DP = 64


def with_ends(array, stream_key, low, largest):
    index_at = [jax.random.randint(jax.random.fold_in(stream_key, axis), (), 0, length) for axis, length in enumerate(array.shape)]
    widest = array.shape.index(max(array.shape))
    next_to = index_at[:widest] + [(index_at[widest] + 1) % array.shape[widest]] + index_at[widest + 1:]
    return array.at[tuple(index_at)].set(low).at[tuple(next_to)].set(largest)


def block_scale(own_key, extent, split, least, high):
    loudness = 1.0
    for position, blocks in split:
        heights = jax.random.uniform(jax.random.fold_in(jax.random.fold_in(own_key, 6), position), (blocks,), jnp.float32, least / len(split), high / len(split))
        loudness = loudness * jnp.repeat(jnp.exp(heights), extent[position] // blocks).reshape((-1,) + (1,) * (len(extent) - 1 - position))
    return loudness


def noise(own_key, dims, scale, reach, pieces=(), kind=jnp.bfloat16):
    entries = jax.random.normal(own_key, dims, jnp.float32) * scale
    if len(pieces) > 0:
        entries = block_scale(own_key, dims, pieces, -0.22, 0.18) * entries
    return jnp.clip(entries, min=-reach, max=reach).astype(kind)


def setup_inputs(seed: int = 0) -> dict:
    seeds = jax.random.split(jax.random.key(seed), 6)
    return {
        "embeddings": noise(seeds[0], (DOCS, D), 1.0, 6.0, ((0, 64),)),
        "valid_mask": with_ends((jax.random.randint(seeds[1], (DOCS,), 0, 4) < 3).astype(jnp.int32), jax.random.fold_in(seeds[1], 1), 0, 1),
        "first_weight": noise(seeds[2], (MEMBERS, D, H), D ** -0.5, 0.1875, ((1, 64), (2, 8))),
        "second_weight": noise(seeds[3], (MEMBERS, H, C), H ** -0.5, 0.09375, ((1, 8),)),
        "thresholds": with_ends(jax.random.randint(seeds[4], (MEMBERS,), -256, 257), jax.random.fold_in(seeds[4], 1), -256, 256).astype(jnp.int32),
    }


def member_logits(embeddings, first_weight, second_weight):
    blocks = embeddings.reshape(N_DP, DOC_DEV, D)

    def one_member(weights):
        layer_one, layer_two = weights

        def one_block(block_rows):
            hidden = jnp.maximum(jnp.dot(block_rows, layer_one, preferred_element_type=jnp.float32), 0.0).astype(jnp.bfloat16)
            return jnp.dot(hidden, layer_two, preferred_element_type=jnp.float32)
        return lax.map(one_block, blocks).reshape(DOCS, C)
    return lax.map(one_member, (first_weight, second_weight))

def reference(embeddings, valid_mask, first_weight, second_weight, thresholds):
    logits = member_logits(embeddings, first_weight, second_weight)
    mean_logits = lax.optimization_barrier(jnp.sum(logits, axis=0)) / MEMBERS
    levels = jnp.arange(C, dtype=jnp.float32)
    grades = (2.0 * levels / (C - 1) - 1.0) * jnp.sqrt(jnp.float32(3.0 / C))
    scores = jnp.einsum('edc,c->ed', logits, grades, precision=lax.Precision.HIGHEST)
    ens_score = jnp.dot(mean_logits, grades, precision=lax.Precision.HIGHEST)
    cutoffs = thresholds.astype(jnp.float32) / 256.0
    validity = valid_mask.astype(jnp.float32)
    kept_soft = validity[None, :] * jax.nn.sigmoid(4.0 * (scores - cutoffs[:, None]))
    ens_kept = jax.nn.sigmoid(4.0 * (ens_score - jnp.mean(cutoffs)))
    kept_share = lax.optimization_barrier(jnp.sum(kept_soft, axis=1)) / DOC_DEV
    agree_share = lax.optimization_barrier(jnp.sum(kept_soft * ens_kept[None, :], axis=1)) / DOC_DEV
    return (mean_logits, kept_share, agree_share)
```

```python
import jax
import jax.numpy as jnp
from jax import lax
from jax.experimental import pallas as pl
from jax.experimental.pallas import tpu as pltpu
from jax.sharding import PartitionSpec as P

MESH = pl.DeviceIdType.MESH
NZ, NX, NC, NY, NH = 8, 4, 2, 4, 2
M, R, F = 8, 16, 512
DOCS, D, G = 768, 1024, 128
BLK = DOCS // NY
FH = F // 2
EARLY = 7
KD = NX * NC * R
FWD_LAG, DOT_LAG = 3, 4
LAST = NZ - 1 + DOT_LAG


def kernel(
    thr, valid, emb, w1, w2, mean_out, kept_out, agree_out,
    W, hid, embv, w2v, w2e, acc, msend, mrecv, zsend, zrecv, scs, scr, szs, szr, st, p1, p2s, p2,
    loc, zr_r, zr_s, zl_r, zl_s, zxr_r, zxr_s, zxl_r, zxl_s,
    xl_r, xr_r, xfl_r, xfr_r, x_s, xxl_r, xxr_r, xxfl_r, xxfr_r, d_r, d_s,
    ylv, zlv, sc_r, sc_s, mr_r, mr_s, szr_r, szr_s, zm_r, zm_s, ag_r, ag_s, p1_r, p1_s, p2_r, p2_s,
):
    dp, ens = lax.axis_index("dp"), lax.axis_index("ens")
    z, x, c = dp // (NX * NC), (dp // NC) % NX, dp % NC
    y, zh = ens // NH, ens % NH

    def dev(z=z, x=x, c=c, y=y, zh=zh):
        return ((z * NX + x) * NC + c, y * NH + zh)

    right, left = (x + 1) % NX, (x + NX - 1) % NX
    ring = zh * NZ + z
    up, down = (ring + 1) % (NZ * NH), (ring + NZ * NH - 1) % (NZ * NH)
    up_dev, down_dev = dev(z=up % NZ, zh=up // NZ), dev(z=down % NZ, zh=down // NZ)
    x_right, x_left = dev(x=right), dev(x=left)
    z_right, z_left = dev(z=(z + 1) % NZ), dev(z=(z + NZ - 1) % NZ)
    partner = dev(c=1 - c)
    across = dev(zh=1 - zh)
    y_up, y_down = dev(y=(y + 1) % NY), dev(y=(y + NY - 1) % NY)
    has_right, has_left = z < NZ - 1, z > 0

    def main(zp, xp, g):
        return W.at[pl.ds(0, EARLY), zp, xp, c, :, pl.ds(g * FH, FH)]

    def late(zp, xp, g):
        return W.at[pl.ds(EARLY, M - EARLY), zp, xp, c, :, pl.ds(g * FH, FH)]

    def late_rows(zp):
        return W.at[pl.ds(EARLY, M - EARLY), zp, :, c]

    def put(ref, send, recv, to, dst=None):
        return pltpu.make_async_remote_copy(
            src_ref=ref, dst_ref=ref if dst is None else dst, send_sem=send, recv_sem=recv,
            device_id=to, device_id_type=MESH)

    def landed(ref, recv):
        put(ref, x_s.at[0], recv, partner).wait_recv()

    def sent(ref, send):
        put(ref, send, d_r.at[0], partner).wait_send()

    barrier = pltpu.get_barrier_semaphore()
    for to in (partner, x_right, x_left, y_up, y_down, up_dev, down_dev):
        pl.semaphore_signal(barrier, inc=1, device_id=to, device_id_type=MESH)
    own_w1 = pltpu.make_async_copy(w1, W.at[:, z, x, c], loc.at[0])
    own_w1.start()
    embs = [pltpu.make_async_copy(emb.at[:, pl.ds(k * KD, KD)], embv.at[k], loc.at[2 + k]) for k in range(NZ)]
    own_w2 = pltpu.make_async_copy(w2, w2v, loc.at[1])
    own_w1.wait()
    pl.semaphore_wait(barrier, 7)

    def send_x(piece, zp, rows, lrecv, rrecv):
        for g in (0, 1):
            put(piece(zp, x, g), x_s.at[0], lrecv.at[rows, g], x_right).start()
            put(piece(zp, x, 1 - g), x_s.at[1], rrecv.at[rows, 1 - g], x_left).start()

    def send_d(ref, zp):
        put(ref, d_s.at[zp], d_r.at[zp], partner).start()

    send_x(late, z, 0, xxl_r, xxr_r)
    for g in (0, 1):
        @pl.when(has_right)
        def _():
            put(main(z, x, g), zr_s.at[0, g], zr_r.at[0, g], z_right).start()

        @pl.when(has_left)
        def _():
            put(main(z, x, g), zl_s.at[0, g], zl_r.at[0, g], z_left).start()
    send_x(main, z, z, xl_r, xr_r)
    for g in (0, 1):
        send_d(main(z, x, g), z)
    pl.semaphore_signal(ylv.at[0], inc=1, device_id=y_up, device_id_type=MESH)
    pl.semaphore_signal(ylv.at[1], inc=1, device_id=y_down, device_id_type=MESH)
    for e in embs:
        e.start()
    own_w2.start()

    def clear(k, carry):
        hid[k // 3, pl.ds((k % 3) * 256, 256), :] = jnp.zeros((256, F), jnp.float32)
        return carry

    lax.fori_loop(0, 3 * M, clear, 0)
    own_w2.wait()

    lane = lax.broadcasted_iota(jnp.int32, (F, G), 1)
    grades = (2.0 * lane.astype(jnp.float32) / (G - 1) - 1.0) * jnp.sqrt(jnp.float32(3.0 / G))

    def extend(e, carry):
        rows = w2v[e]
        col = jnp.sum(rows.astype(jnp.float32) * grades, axis=1, keepdims=True)
        hi = col.astype(jnp.bfloat16).astype(jnp.float32)
        mid = (col - hi).astype(jnp.bfloat16).astype(jnp.float32)
        low = col - hi - mid
        part = jnp.where(lane == e, hi, 0.0) + jnp.where(lane == e + M, mid, 0.0) + jnp.where(lane == e + 2 * M, low, 0.0)
        w2e[e, :, :G] = rows
        w2e[e, :, G:] = part.astype(jnp.bfloat16)
        return carry

    lax.fori_loop(0, M, extend, 0)
    for e in embs:
        e.wait()
    pl.semaphore_wait(ylv.at[0], 1)
    pl.semaphore_wait(ylv.at[1], 1)

    near = jnp.minimum(z, NZ - 1 - z)

    def order(i):
        s = (i + 1) // 2
        both = jnp.where(i % 2 == 1, z - s, z + s)
        return jnp.where(i <= 2 * near, both, jnp.where(z < NZ // 2, i, NZ - 1 - i))

    def z_stage(t, zp, there, on, onward, recv, send):
        @pl.when((t < NZ) & there)
        def _():
            for g in (0, 1):
                landed(main(zp, x, g), recv.at[t - 1, g])

                @pl.when(on)
                def _():
                    put(main(zp, x, g), send.at[t, g], recv.at[t, g], onward).start()
            send_x(main, zp, zp, xl_r, xr_r)
            for g in (0, 1):
                send_d(main(zp, x, g), zp)

    def late_stage(s, zp, there, on, onward, recv, send):
        @pl.when((s >= 1) & (s < NZ) & there)
        def _():
            landed(late_rows(zp), recv.at[s - 1])

            @pl.when(on)
            def _():
                put(late_rows(zp), send.at[s], recv.at[s], onward).start()
            send_d(late_rows(zp), zp)

    def step(t, carry):
        @pl.when(t < NZ)
        def _():
            pl.semaphore_signal(zlv.at[0], inc=1, device_id=up_dev, device_id_type=MESH)
            pl.semaphore_signal(zlv.at[1], inc=1, device_id=down_dev, device_id_type=MESH)
        z_stage(t, z - t, z - t >= 0, has_right, z_right, zr_r, zr_s)
        z_stage(t, z + t, z + t < NZ, has_left, z_left, zl_r, zl_s)

        @pl.when(t == 1)
        def _():
            landed(late(z, left, 0), xxl_r.at[0, 0])
            put(late(z, left, 0), x_s.at[2], xxfl_r.at[0], x_right).start()
            landed(late(z, right, 1), xxr_r.at[0, 1])
            put(late(z, right, 1), x_s.at[3], xxfr_r.at[0], x_left).start()
            landed(late(z, left, 1), xxl_r.at[0, 1])
            landed(late(z, right, 0), xxr_r.at[0, 0])
            landed(late(z, (x + 2) % NX, 0), xxfl_r.at[0])
            landed(late(z, (x + 2) % NX, 1), xxfr_r.at[0])

            @pl.when(has_right)
            def _():
                put(late_rows(z), zxr_s.at[0], zxr_r.at[0], z_right).start()

            @pl.when(has_left)
            def _():
                put(late_rows(z), zxl_s.at[0], zxl_r.at[0], z_left).start()
            send_d(late_rows(z), z)

        late_stage(t - 1, z - t + 1, z - t + 1 >= 0, has_right, z_right, zxr_r, zxr_s)
        late_stage(t - 1, z + t - 1, z + t - 1 < NZ, has_left, z_left, zxl_r, zxl_s)

        @pl.when(t <= NZ)
        def _():
            zp = order(t - 1)
            landed(main(zp, left, 0), xl_r.at[zp, 0])
            put(main(zp, left, 0), x_s.at[2], xfl_r.at[zp], x_right).start()
            landed(main(zp, right, 1), xr_r.at[zp, 1])
            put(main(zp, right, 1), x_s.at[3], xfr_r.at[zp], x_left).start()
            landed(main(zp, left, 1), xl_r.at[zp, 1])
            landed(main(zp, right, 0), xr_r.at[zp, 0])
            for g in (0, 1):
                send_d(main(zp, left, g), zp)
                send_d(main(zp, right, g), zp)

        @pl.when((t >= FWD_LAG) & (t < NZ + FWD_LAG))
        def _():
            zp = order(t - FWD_LAG)
            landed(main(zp, (x + 2) % NX, 0), xfl_r.at[zp])
            landed(main(zp, (x + 2) % NX, 1), xfr_r.at[zp])
            for g in (0, 1):
                send_d(main(zp, (x + 2) % NX, g), zp)

        @pl.when((t >= DOT_LAG) & (t < NZ + DOT_LAG))
        def _():
            zp = order(t - DOT_LAG)
            landed(W.at[:, zp, :, 1 - c], d_r.at[zp])

            def one(k, carry):
                e, rows = k // 3, pl.ds((k % 3) * 256, 256)
                block = W[e, zp].reshape(KD, F)
                hid[e, rows, :] += jnp.dot(embv[zp, rows, :], block, preferred_element_type=jnp.float32)
                return carry

            lax.fori_loop(0, 3 * M, one, 0)

        @pl.when(t < NZ)
        def _():
            pl.semaphore_wait(zlv.at[0], 1)
            pl.semaphore_wait(zlv.at[1], 1)
        return carry

    lax.fori_loop(1, LAST + 1, step, 0)

    acc[pl.ds(DOCS, 64), :] = jnp.zeros((64, 2 * G), jnp.float32)

    def second(k, carry):
        rows = pl.ds(k * 128, 128)
        total = None
        for e in range(M):
            h = jnp.maximum(hid[e, rows, :], 0.0).astype(jnp.bfloat16)
            p = jnp.dot(h, w2e[e], preferred_element_type=jnp.float32)
            total = p if total is None else total + p
        acc[rows, :] = total
        msend[rows, :] = total[:, :G].astype(jnp.bfloat16)
        return carry

    lax.fori_loop(0, DOCS // 128, second, 0)

    for k in range(NY):
        cols = acc[pl.ds(k * BLK, 256), G:].T
        scs[k] = cols[0:M] + cols[M:2 * M] + cols[2 * M:3 * M]

    def y_peer(k):
        return (y + k) % NY

    def y_rows(k):
        return pl.ds(pl.multiple_of(k * BLK, BLK), BLK)

    for k in range(1, NY):
        put(scs.at[y_peer(k)], sc_s, sc_r, dev(y=y_peer(k)), scr.at[y]).start()
    for k in range(1, NY):
        put(msend.at[y_rows(y_peer(k))], mr_s, mr_r, dev(y=y_peer(k)), mrecv.at[y]).start()

    landed(scr.at[pl.ds(0, NY - 1)], sc_r)
    szs[...] = scs[y] + (scr[y_peer(1)] + scr[y_peer(2)] + scr[y_peer(3)])
    put(szs, szr_s, szr_r, across, szr).start()

    landed(mrecv.at[pl.ds(0, NY - 1)], mr_r)
    part = acc[y_rows(y), :G]
    for k in range(1, NY):
        part = part + mrecv[y_peer(k)].astype(jnp.float32)
    zsend[...] = part.astype(jnp.bfloat16)
    put(zsend, zm_s, zm_r, across, zrecv).start()

    member = lax.broadcasted_iota(jnp.int32, (M, 1), 0)
    cut, mean_cut = jnp.zeros((M, 1), jnp.float32), 0.0
    for e in range(M):
        te = thr[e].astype(jnp.float32) / 256.0
        cut = jnp.where(member == e, te, cut)
        mean_cut = mean_cut + te
    mean_cut = mean_cut / M
    landed(szr, szr_r)
    scores = szs[...] + szr[...]
    kept = valid[pl.ds(y, 1), :] * jax.nn.sigmoid(4.0 * (scores - cut))
    ens_score = jnp.sum(scores, axis=0, keepdims=True) / M
    agree = kept * jax.nn.sigmoid(4.0 * (ens_score - mean_cut))
    kept_sum = jnp.sum(kept, axis=1, keepdims=True)
    agree_sum = jnp.sum(agree, axis=1, keepdims=True)
    lane8 = lax.broadcasted_iota(jnp.int32, (M, G), 1)
    table = jnp.where(lane8 == 0, kept_sum, jnp.where(lane8 == 1, agree_sum, 0.0))
    for e in range(M):
        st[e] = table[e:e + 1]
    mine = (y * NX + x) * NC + c
    p1[mine] = st[ens]

    def share(k, carry):
        q = (mine + k) % (NY * NX * NC)
        yp, xp, cp = q // (NX * NC), (q // NC) % NX, q % NC
        put(st.at[yp * NH + zh], p1_s, p1_r, dev(y=yp, x=xp, c=cp), p1.at[mine]).start()
        return carry

    lax.fori_loop(1, NY * NX * NC, share, 0)

    landed(zrecv, zm_r)
    mean_out[y_rows(y), :] = (zsend[...].astype(jnp.float32) + zrecv[...].astype(jnp.float32)) * (1.0 / M)
    for k in range(1, NY):
        put(mean_out.at[y_rows(y)], ag_s, ag_r, dev(y=y_peer(k))).start()

    landed(p1.at[pl.ds(0, NY * NX * NC - 1)], p1_r)
    p2s[...] = jnp.sum(p1[...], axis=0)
    p2[z] = p2s[...]
    for k in range(1, NZ):
        put(p2s, p2_s, p2_r, dev(z=(z + k) % NZ), p2.at[z]).start()

    landed(mean_out.at[pl.ds(0, DOCS - BLK)], ag_r)
    landed(p2.at[pl.ds(0, NZ - 1)], p2_r)
    total = jnp.sum(p2[...], axis=0) * (1.0 / DOCS)
    kept_out[0] = total[0, 0]
    agree_out[0] = total[0, 1]

    for s in range(NZ - 1):
        @pl.when(has_right & (s <= z))
        def _():
            for g in (0, 1):
                sent(main(0, 0, g), zr_s.at[s, g])
            sent(late_rows(0), zxr_s.at[s])

        @pl.when(has_left & (z + s < NZ))
        def _():
            for g in (0, 1):
                sent(main(0, 0, g), zl_s.at[s, g])
            sent(late_rows(0), zxl_s.at[s])
    for k in (0, 1):
        sent(W.at[pl.ds(0, EARLY), :, 0, 0], x_s.at[k])
        sent(W.at[pl.ds(EARLY, M - EARLY), 0, 0, 0], x_s.at[k])
        sent(W.at[pl.ds(0, EARLY), :, 0, 0, :, pl.ds(0, FH)], x_s.at[2 + k])
        sent(W.at[pl.ds(EARLY, M - EARLY), 0, 0, 0, :, pl.ds(0, FH)], x_s.at[2 + k])
    for k in range(NZ):
        sent(W.at[:, k, :, 0], d_s.at[k])
    sent(scr.at[pl.ds(0, NY - 1)], sc_s)
    sent(mrecv.at[pl.ds(0, NY - 1)], mr_s)
    sent(szs, szr_s)
    sent(zsend, zm_s)
    sent(mean_out.at[pl.ds(0, DOCS - BLK)], ag_s)
    sent(p1.at[pl.ds(0, NY * NX * NC - 1)], p1_s)
    sent(p2.at[pl.ds(0, NZ - 1)], p2_s)


def on_device(embeddings, valid_mask, first_weight, second_weight, thresholds):
    valid = jnp.pad(valid_mask.reshape(NY, BLK).astype(jnp.float32), ((0, 0), (0, 256 - BLK)))
    dma, reg = pltpu.SemaphoreType.DMA, pltpu.SemaphoreType.REGULAR
    f32, bf16 = jnp.float32, jnp.bfloat16
    vmem = pl.BlockSpec(memory_space=pltpu.VMEM)
    smem = pl.BlockSpec(memory_space=pltpu.SMEM)
    hbm = pl.BlockSpec(memory_space=pl.ANY)
    mean, kept, agree = pl.pallas_call(
        kernel,
        out_shape=(
            jax.ShapeDtypeStruct((DOCS, G), f32),
            jax.ShapeDtypeStruct((1,), f32),
            jax.ShapeDtypeStruct((1,), f32),
        ),
        in_specs=[smem, vmem, hbm, hbm, hbm],
        out_specs=(vmem, smem, smem),
        scratch_shapes=[
            pltpu.VMEM((M, NZ, NX, NC, R, F), bf16),
            pltpu.VMEM((M, DOCS, F), f32),
            pltpu.VMEM((NZ, DOCS, KD), bf16),
            pltpu.VMEM((M, F, G), bf16),
            pltpu.VMEM((M, F, 2 * G), bf16),
            pltpu.VMEM((DOCS + 64, 2 * G), f32),
            pltpu.VMEM((DOCS, G), bf16),
            pltpu.VMEM((NY, BLK, G), bf16),
            pltpu.VMEM((BLK, G), bf16),
            pltpu.VMEM((BLK, G), bf16),
            pltpu.VMEM((NY, M, 256), f32),
            pltpu.VMEM((NY, M, 256), f32),
            pltpu.VMEM((M, 256), f32),
            pltpu.VMEM((M, 256), f32),
            pltpu.VMEM((M, 1, G), f32),
            pltpu.VMEM((NY * NX * NC, 1, G), f32),
            pltpu.VMEM((1, G), f32),
            pltpu.VMEM((NZ, 1, G), f32),
            dma((2 + NZ,)),
            dma((NZ, 2)), dma((NZ, 2)), dma((NZ, 2)), dma((NZ, 2)),
            dma((NZ,)), dma((NZ,)), dma((NZ,)), dma((NZ,)),
            dma((NZ, 2)), dma((NZ, 2)), dma((NZ,)), dma((NZ,)), dma((4,)),
            dma((1, 2)), dma((1, 2)), dma((1,)), dma((1,)), dma((NZ,)), dma((NZ,)),
            reg((2,)), reg((2,)),
            dma, dma, dma, dma, dma, dma, dma, dma, dma, dma, dma, dma, dma, dma,
        ],
        compiler_params=pltpu.CompilerParams(
            collective_id=0, has_side_effects=True, vmem_limit_bytes=56 * 1024 * 1024
        ),
    )(thresholds, valid, embeddings, first_weight, second_weight)
    return mean, kept, agree


def solution(mesh):
    return jax.shard_map(
        on_device,
        mesh=mesh,
        in_specs=(P("dp", None), P("dp"), P(None, "dp", "ens"), P(None, "ens", None), P()),
        out_specs=(P("dp", None), P("ens"), P("ens")),
        check_vma=False,
    )
```

```python
import jax
import jax.numpy as jnp
from jax import lax
from jax.experimental import pallas as pl
from jax.experimental.pallas import tpu as pltpu
from jax.sharding import PartitionSpec as P

MESH = pl.DeviceIdType.MESH
NZ, NX, NC, NY, NH = 8, 4, 2, 4, 2
M, R, F = 8, 16, 512
DOCS, D, G = 768, 1024, 128
BLK = DOCS // NY
FH = F // 2
EARLY = 7
KD = NX * NC * R
FWD_LAG, DOT_LAG = 3, 5
LAST = DOT_LAG + NZ - 3


def kernel(
    thr_in, valid_in, emb, w1, w2, mean_out, kept_out, agree_out,
    thr, valid, W, hid, embv, w2v, w2e, acc, window, msend, mrecv, zsend, zrecv, whole, scs, scr, szs, szr, st, p1, p2s, p2,
    loc, zr_r, zr_s, zl_r, zl_s, zxr_r, zxr_s, zxl_r, zxl_s,
    xl_r, xr_r, xfl_r, xfr_r, x_s, xxl_r, xxr_r, xxfl_r, xxfr_r, d_r, d_s,
    ylv, zlv, sc_r, sc_s, mr_r, mr_s, szr_r, szr_s, zm_r, zm_s, ag_r, ag_s, p1_r, p1_s, p2_r, p2_s,
):
    dp, ens = lax.axis_index("dp"), lax.axis_index("ens")
    z, x, c = dp // (NX * NC), (dp // NC) % NX, dp % NC
    y, zh = ens // NH, ens % NH

    def dev(z=z, x=x, c=c, y=y, zh=zh):
        return ((z * NX + x) * NC + c, y * NH + zh)

    right, left = (x + 1) % NX, (x + NX - 1) % NX
    ring = zh * NZ + z
    up, down = (ring + 1) % (NZ * NH), (ring + NZ * NH - 1) % (NZ * NH)
    up_dev, down_dev = dev(z=up % NZ, zh=up // NZ), dev(z=down % NZ, zh=down // NZ)
    x_right, x_left = dev(x=right), dev(x=left)
    z_right, z_left = dev(z=(z + 1) % NZ), dev(z=(z + NZ - 1) % NZ)
    partner = dev(c=1 - c)
    across = dev(zh=1 - zh)
    y_up, y_down = dev(y=(y + 1) % NY), dev(y=(y + NY - 1) % NY)
    has_right, has_left = z < NZ - 1, z > 0

    def main(zp, xp, g):
        return W.at[pl.ds(0, EARLY), zp, xp, c, :, pl.ds(g * FH, FH)]

    def shard(zp, xp):
        return W.at[pl.ds(0, EARLY), zp, xp, c]

    def late(zp, xp, g):
        return W.at[pl.ds(EARLY, M - EARLY), zp, xp, c, :, pl.ds(g * FH, FH)]

    def late_rows(zp):
        return W.at[pl.ds(EARLY, M - EARLY), zp, :, c]

    def put(ref, send, recv, to, dst=None):
        return pltpu.make_async_remote_copy(
            src_ref=ref, dst_ref=ref if dst is None else dst, send_sem=send, recv_sem=recv,
            device_id=to, device_id_type=MESH)

    def landed(ref, recv):
        put(ref, x_s.at[0], recv, partner).wait_recv()

    def sent(ref, send):
        put(ref, send, d_r.at[0], partner).wait_send()

    barrier = pltpu.get_barrier_semaphore()
    for to in (partner, x_right, x_left, y_up, y_down, up_dev, down_dev):
        pl.semaphore_signal(barrier, inc=1, device_id=to, device_id_type=MESH)
    own_w1 = pltpu.make_async_copy(w1, W.at[:, z, x, c], loc.at[0])
    own_w1.start()
    embs = [pltpu.make_async_copy(emb.at[:, pl.ds(k * KD, KD)], embv.at[k], loc.at[2 + k]) for k in range(NZ)]
    own_w2 = pltpu.make_async_copy(w2, w2v, loc.at[1])
    small = [pltpu.make_async_copy(thr_in, thr, loc.at[2 + NZ]), pltpu.make_async_copy(valid_in, valid, loc.at[3 + NZ])]
    own_w1.wait()
    pl.semaphore_wait(barrier, 7)

    def send_x(piece, zp, rows, lrecv, rrecv):
        for g in (0, 1):
            put(piece(zp, x, g), x_s.at[0], lrecv.at[rows, g], x_right).start()
            put(piece(zp, x, 1 - g), x_s.at[1], rrecv.at[rows, 1 - g], x_left).start()

    def send_d(ref, zp):
        put(ref, d_s.at[zp], d_r.at[zp], partner).start()

    send_x(late, z, 0, xxl_r, xxr_r)
    for g in (0, 1):
        @pl.when(has_right)
        def _():
            put(main(z, x, g), zr_s.at[0, g], zr_r.at[0, g], z_right).start()

        @pl.when(has_left)
        def _():
            put(main(z, x, g), zl_s.at[0, g], zl_r.at[0, g], z_left).start()
    send_x(main, z, z, xl_r, xr_r)
    send_d(shard(z, x), z)
    pl.semaphore_signal(ylv.at[0], inc=1, device_id=y_up, device_id_type=MESH)
    pl.semaphore_signal(ylv.at[1], inc=1, device_id=y_down, device_id_type=MESH)
    for e in embs:
        e.start()
    own_w2.start()
    for e in small:
        e.start()

    def clear(k, carry):
        hid[k // 3, pl.ds((k % 3) * 256, 256), :] = jnp.zeros((256, F), jnp.float32)
        return carry

    lax.fori_loop(0, 3 * M, clear, 0)
    window[...] = jnp.zeros((2 * G, G), jnp.float32)
    own_w2.wait()

    lane = lax.broadcasted_iota(jnp.int32, (F, G), 1)
    grades = (2.0 * lane.astype(jnp.float32) / (G - 1) - 1.0) * jnp.sqrt(jnp.float32(3.0 / G))

    def extend(e, carry):
        rows = w2v[e]
        col = jnp.sum(rows.astype(jnp.float32) * grades, axis=1, keepdims=True)
        hi = col.astype(jnp.bfloat16).astype(jnp.float32)
        mid = (col - hi).astype(jnp.bfloat16).astype(jnp.float32)
        low = col - hi - mid
        at = (e % NH) * NY + e // NH
        part = jnp.where(lane == at, hi, 0.0) + jnp.where(lane == at + M, mid, 0.0) + jnp.where(lane == at + 2 * M, low, 0.0)
        w2e[e, :, :G] = rows
        w2e[e, :, G:] = part.astype(jnp.bfloat16)
        return carry

    lax.fori_loop(0, M, extend, 0)
    landed(late(z, left, 0), xxl_r.at[0, 0])
    put(late(z, left, 0), x_s.at[2], xxfl_r.at[0], x_right).start()
    landed(late(z, right, 1), xxr_r.at[0, 1])
    put(late(z, right, 1), x_s.at[3], xxfr_r.at[0], x_left).start()
    pl.semaphore_wait(ylv.at[0], 1)
    pl.semaphore_wait(ylv.at[1], 1)

    near = jnp.minimum(z, NZ - 1 - z)

    def order(i):
        s = (i + 1) // 2
        both = jnp.where(i % 2 == 1, z - s, z + s)
        return jnp.where(i <= 2 * near, both, jnp.where(z < NZ // 2, i, NZ - 1 - i))

    def z_stage(t, zp, there, on, onward, recv, send):
        @pl.when((t < NZ) & there)
        def _():
            for g in (0, 1):
                landed(main(zp, x, g), recv.at[t - 1, g])

                @pl.when(on)
                def _():
                    put(main(zp, x, g), send.at[t, g], recv.at[t, g], onward).start()
            send_x(main, zp, zp, xl_r, xr_r)
            send_d(shard(zp, x), zp)

    def late_stage(s, zp, there, on, onward, recv, send):
        @pl.when((s >= 1) & (s < NZ) & there)
        def _():
            landed(late_rows(zp), recv.at[s - 1])

            @pl.when(on)
            def _():
                put(late_rows(zp), send.at[s], recv.at[s], onward).start()
            send_d(late_rows(zp), zp)

    def joined(p):
        for zp in (order(2 * p), order(2 * p + 1)):
            landed(W.at[:, zp, :, 1 - c], d_r.at[zp])

    def dots(p, e):
        za, zb = order(2 * p), order(2 * p + 1)
        block = jnp.concatenate([W[e, za].reshape(KD, F), W[e, zb].reshape(KD, F)], axis=0)

        lhs = jnp.concatenate([embv[za], embv[zb]], axis=1)
        hid[e] += jnp.dot(lhs, block, preferred_element_type=jnp.float32)

    def quarter(t, j):
        @pl.when(t >= DOT_LAG)
        def _():
            p, half = (t - DOT_LAG) // 2, (t - DOT_LAG) % 2
            if j == 0:
                @pl.when(t == DOT_LAG)
                def _():
                    for e in embs + small:
                        e.wait()

                @pl.when(half == 0)
                def _():
                    joined(p)
            dots(p, half * (M // 2) + j)

    def step(t, carry):
        @pl.when(t < NZ)
        def _():
            pl.semaphore_signal(zlv.at[0], inc=1, device_id=up_dev, device_id_type=MESH)
            pl.semaphore_signal(zlv.at[1], inc=1, device_id=down_dev, device_id_type=MESH)
        z_stage(t, z - t, z - t >= 0, has_right, z_right, zr_r, zr_s)
        z_stage(t, z + t, z + t < NZ, has_left, z_left, zl_r, zl_s)

        quarter(t, 0)

        late_stage(t - 1, z - t + 1, z - t + 1 >= 0, has_right, z_right, zxr_r, zxr_s)
        late_stage(t - 1, z + t - 1, z + t - 1 < NZ, has_left, z_left, zxl_r, zxl_s)

        quarter(t, 1)

        @pl.when(t <= NZ)
        def _():
            zp = order(t - 1)
            landed(main(zp, left, 0), xl_r.at[zp, 0])
            put(main(zp, left, 0), x_s.at[2], xfl_r.at[zp], x_right).start()
            landed(main(zp, right, 1), xr_r.at[zp, 1])
            put(main(zp, right, 1), x_s.at[3], xfr_r.at[zp], x_left).start()
            landed(main(zp, left, 1), xl_r.at[zp, 1])
            landed(main(zp, right, 0), xr_r.at[zp, 0])
            send_d(shard(zp, left), zp)
            send_d(shard(zp, right), zp)

        quarter(t, 2)

        @pl.when((t >= FWD_LAG) & (t < NZ + FWD_LAG))
        def _():
            zp = order(t - FWD_LAG)
            landed(main(zp, (x + 2) % NX, 0), xfl_r.at[zp])
            landed(main(zp, (x + 2) % NX, 1), xfr_r.at[zp])
            send_d(shard(zp, (x + 2) % NX), zp)

        @pl.when(t == 1)
        def _():
            landed(late(z, left, 1), xxl_r.at[0, 1])
            landed(late(z, right, 0), xxr_r.at[0, 0])
            landed(late(z, (x + 2) % NX, 0), xxfl_r.at[0])
            landed(late(z, (x + 2) % NX, 1), xxfr_r.at[0])

            @pl.when(has_right)
            def _():
                put(late_rows(z), zxr_s.at[0], zxr_r.at[0], z_right).start()

            @pl.when(has_left)
            def _():
                put(late_rows(z), zxl_s.at[0], zxl_r.at[0], z_left).start()
            send_d(late_rows(z), z)

        @pl.when(t < NZ)
        def _():
            pl.semaphore_wait(zlv.at[0], 1)
            pl.semaphore_wait(zlv.at[1], 1)
        quarter(t, 3)
        return carry

    lax.fori_loop(1, LAST + 1, step, 0)
    joined(NZ // 2 - 1)

    def y_peer(k):
        return (y + k) % NY

    def last(i, carry):
        b = y_peer(jnp.where(i == 0, 2, jnp.where(i == 1, 1, jnp.where(i == 2, 3, 0))))
        rows = pl.ds(pl.multiple_of(b * BLK, BLK), BLK)
        za, zb = order(NZ - 2), order(NZ - 1)
        lhs = jnp.concatenate([embv[za, rows, :], embv[zb, rows, :]], axis=1)
        total = None
        for e in range(M):
            block = jnp.concatenate([W[e, za].reshape(KD, F), W[e, zb].reshape(KD, F)], axis=0)
            pre = hid[e, rows, :] + jnp.dot(lhs, block, preferred_element_type=jnp.float32)
            h = jnp.maximum(pre, 0.0).astype(jnp.bfloat16)
            p = jnp.dot(h, w2e[e], preferred_element_type=jnp.float32)
            total = p if total is None else total + p
        acc[...] = total[:, :G]
        msend[b] = total[:, :G].astype(jnp.bfloat16)
        window[pl.ds(pl.multiple_of((b % 2) * (2 * G - BLK), 2 * G - BLK), BLK), :] = total[:, G:]
        cols = window[...].T
        scs[b] = cols[0:M] + cols[M:2 * M] + cols[2 * M:3 * M]

        @pl.when(i < NY - 1)
        def _():
            put(scs.at[b], sc_s, sc_r, dev(y=b), scr.at[y]).start()
            put(msend.at[b], mr_s, mr_r, dev(y=b), mrecv.at[y]).start()
        return carry

    lax.fori_loop(0, NY, last, 0)

    landed(scr.at[pl.ds(0, NY - 1)], sc_r)
    mine_y = scs[y] + (scr[y_peer(1)] + scr[y_peer(2)] + scr[y_peer(3)])
    row = y * BLK // G
    lane2 = lax.broadcasted_iota(jnp.int32, (1, 2 * G), 1)
    first = (y % 2) * (2 * G - BLK)
    inside = (lane2 >= first) & (lane2 < first + BLK)
    flags = jnp.concatenate([valid[pl.ds(row, 1), :], valid[pl.ds(row + 1, 1), :]], axis=1).astype(jnp.float32)
    flags = jnp.where(inside, flags, 0.0)
    every = jnp.sum(mine_y, axis=0, keepdims=True)
    half_way = (z + NZ // 2) % NZ
    for h in range(NH):
        szs[h] = jnp.concatenate(
            [mine_y[h * NY:(h + 1) * NY], every, flags, jnp.zeros((2, 2 * G), jnp.float32)], axis=0)
        put(szs.at[h], szr_s, szr_r, dev(z=half_way, zh=h), szr.at[zh]).start()

    landed(mrecv.at[pl.ds(0, NY - 1)], mr_r)
    part = acc[...]
    for k in range(1, NY):
        part = part + mrecv[y_peer(k)].astype(jnp.float32)
    zsend[...] = part.astype(jnp.bfloat16)
    put(zsend, zm_s, zm_r, across, zrecv).start()

    member = lax.broadcasted_iota(jnp.int32, (NY, 1), 0)
    cut, mean_cut = jnp.zeros((NY, 1), jnp.float32), 0.0
    for e in range(M):
        te = thr[e].astype(jnp.float32) / 256.0
        cut = jnp.where((member == e // NH) & (zh == e % NH), te, cut)
        mean_cut = mean_cut + te
    mean_cut = mean_cut / M
    landed(szr, szr_r)
    scores = szr[0] + szr[1]
    kept = szr[0, NY + 1:NY + 2] * jax.nn.sigmoid(4.0 * (scores[0:NY] - cut))
    agree = kept * jax.nn.sigmoid(4.0 * (scores[NY:NY + 1] / M - mean_cut))
    kept_sum = jnp.sum(kept, axis=1, keepdims=True)
    agree_sum = jnp.sum(agree, axis=1, keepdims=True)
    lane4 = lax.broadcasted_iota(jnp.int32, (NY, G), 1)
    table = jnp.where(lane4 == 0, kept_sum, jnp.where(lane4 == 1, agree_sum, 0.0))
    for k in range(NY):
        st[k] = table[k:k + 1]
    mine = (y * NX + x) * NC + c
    p1[mine] = st[y]

    def share(k, carry):
        q = (mine + k) % (NY * NX * NC)
        yp, xp, cp = q // (NX * NC), (q // NC) % NX, q % NC
        put(st.at[yp], p1_s, p1_r, dev(y=yp, x=xp, c=cp), p1.at[mine]).start()
        return carry

    lax.fori_loop(1, NY * NX * NC, share, 0)

    landed(zrecv, zm_r)
    whole[y] = ((zsend[...].astype(jnp.float32) + zrecv[...].astype(jnp.float32)) * (1.0 / M)).astype(jnp.bfloat16)
    for k in range(1, NY):
        put(whole.at[y], ag_s, ag_r, dev(y=y_peer(k))).start()

    landed(p1.at[pl.ds(0, NY * NX * NC - 1)], p1_r)
    p2s[...] = jnp.sum(p1[...], axis=0)
    p2[z] = p2s[...]
    for k in range(1, NZ):
        put(p2s, p2_s, p2_r, dev(z=(z + k) % NZ), p2.at[z]).start()

    landed(whole.at[pl.ds(0, NY - 1)], ag_r)
    out = pltpu.make_async_copy(whole, mean_out, loc.at[0])
    out.start()
    landed(p2.at[pl.ds(0, NZ - 1)], p2_r)
    total = jnp.sum(p2[...], axis=0) * (1.0 / DOCS)
    kept_out[0] = total[0, 0]
    agree_out[0] = total[0, 1]

    out.wait()

    for s in range(NZ - 1):
        @pl.when(has_right & (s <= z))
        def _():
            for g in (0, 1):
                sent(main(0, 0, g), zr_s.at[s, g])
            sent(late_rows(0), zxr_s.at[s])

        @pl.when(has_left & (z + s < NZ))
        def _():
            for g in (0, 1):
                sent(main(0, 0, g), zl_s.at[s, g])
            sent(late_rows(0), zxl_s.at[s])
    for k in (0, 1):
        sent(W.at[pl.ds(0, EARLY), :, 0, 0], x_s.at[k])
        sent(W.at[pl.ds(EARLY, M - EARLY), 0, 0, 0], x_s.at[k])
        sent(W.at[pl.ds(0, EARLY), :, 0, 0, :, pl.ds(0, FH)], x_s.at[2 + k])
        sent(W.at[pl.ds(EARLY, M - EARLY), 0, 0, 0, :, pl.ds(0, FH)], x_s.at[2 + k])
    for k in range(NZ):
        sent(W.at[:, k, :, 0], d_s.at[k])
    sent(scr.at[pl.ds(0, NY - 1)], sc_s)
    sent(mrecv.at[pl.ds(0, NY - 1)], mr_s)
    sent(szs, szr_s)
    sent(zsend, zm_s)
    sent(whole.at[pl.ds(0, NY - 1)], ag_s)
    sent(p1.at[pl.ds(0, NY * NX * NC - 1)], p1_s)
    sent(p2.at[pl.ds(0, NZ - 1)], p2_s)


def on_device(embeddings, valid_mask, first_weight, second_weight, thresholds):
    valid = valid_mask.reshape(DOCS // G, G)
    dma, reg = pltpu.SemaphoreType.DMA, pltpu.SemaphoreType.REGULAR
    f32, bf16 = jnp.float32, jnp.bfloat16
    smem = pl.BlockSpec(memory_space=pltpu.SMEM)
    hbm = pl.BlockSpec(memory_space=pltpu.HBM)
    mean, kept, agree = pl.pallas_call(
        kernel,
        out_shape=(
            jax.ShapeDtypeStruct((NY, BLK, G), bf16),
            jax.ShapeDtypeStruct((1,), f32),
            jax.ShapeDtypeStruct((1,), f32),
        ),
        in_specs=[hbm] * 5,
        out_specs=(hbm, smem, smem),
        scratch_shapes=[
            pltpu.SMEM((M,), jnp.int32),
            pltpu.VMEM((DOCS // G, G), jnp.int32),
            pltpu.VMEM((M, NZ, NX, NC, R, F), bf16),
            pltpu.VMEM((M, DOCS, F), f32),
            pltpu.VMEM((NZ, DOCS, KD), bf16),
            pltpu.VMEM((M, F, G), bf16),
            pltpu.VMEM((M, F, 2 * G), bf16),
            pltpu.VMEM((BLK, G), f32),
            pltpu.VMEM((2 * G, G), f32),
            pltpu.VMEM((NY, BLK, G), bf16),
            pltpu.VMEM((NY, BLK, G), bf16),
            pltpu.VMEM((BLK, G), bf16),
            pltpu.VMEM((BLK, G), bf16),
            pltpu.VMEM((NY, BLK, G), bf16),
            pltpu.VMEM((NY, M, 256), f32),
            pltpu.VMEM((NY, M, 256), f32),
            pltpu.VMEM((NH, M, 256), f32),
            pltpu.VMEM((NH, M, 256), f32),
            pltpu.VMEM((NY, 1, G), f32),
            pltpu.VMEM((NY * NX * NC, 1, G), f32),
            pltpu.VMEM((1, G), f32),
            pltpu.VMEM((NZ, 1, G), f32),
            dma((4 + NZ,)),
            dma((NZ, 2)), dma((NZ, 2)), dma((NZ, 2)), dma((NZ, 2)),
            dma((NZ,)), dma((NZ,)), dma((NZ,)), dma((NZ,)),
            dma((NZ, 2)), dma((NZ, 2)), dma((NZ,)), dma((NZ,)), dma((4,)),
            dma((1, 2)), dma((1, 2)), dma((1,)), dma((1,)), dma((NZ,)), dma((NZ,)),
            reg((2,)), reg((2,)),
            dma, dma, dma, dma, dma, dma, dma, dma, dma, dma, dma, dma, dma, dma,
        ],
        compiler_params=pltpu.CompilerParams(
            collective_id=0, has_side_effects=True, vmem_limit_bytes=60 * 1024 * 1024
        ),
    )(thresholds, valid, embeddings, first_weight, second_weight)
    return mean.reshape(DOCS, G).astype(f32), kept, agree


def solution(mesh):
    return jax.shard_map(
        on_device,
        mesh=mesh,
        in_specs=(P("dp", None), P("dp"), P(None, "dp", "ens"), P(None, "ens", None), P()),
        out_specs=(P("dp", None), P("ens"), P("ens")),
        check_vma=False,
    )
```
